128 devices in a mesh: north: 32 (over z_hi, y, x), deep: 4 (over z_lo, core).
Axes of the slice: x: 4, y: 4, z: 4 (z_hi: 2, z_lo: 2; z = z_hi * 2 + z_lo), core: 2. Of those that a mesh axis runs over, the one named last changes fastest.
Arguments:
- forcing: float32 [2, 512, 512, 256], P(None, None, 'north', 'deep'), may hold values from -6 to 6
- symbol_x: float32 [512], replicated, may hold values from 0.3 to 3
- symbol_y: float32 [512], replicated, may hold values from 0.3 to 3
- symbol_z: float32 [256], replicated, may hold values from 0.3 to 3
Outputs:
- coefficients: float32 [2, 512, 512, 256], P(None, 'north', 'deep')
The draws below stay inside these ranges and needn't reach their ends.
All inputs are finite; a program needn't handle non-finite values.
Results may differ from the reference program's by a relative error of at most 0.000084.
Values sent between devices are 32-bit elements; how exact they have to be, the bound alone decides.
A program may use at most 64 MiB of HBM per device.

```python
import jax
import jax.numpy as jnp
from jax import lax

GRID_X = 512
GRID_Y = 512
GRID_Z = 256
FIELDS = 2


def block_levels(rng, shape, pieces, least, largest):
    level, own = 1.0, jax.random.fold_in(rng, 6)
    for axis_at, blocks in pieces:
        steps = jnp.exp(jax.random.uniform(jax.random.fold_in(own, axis_at), (blocks,), jnp.float32, least / len(pieces), largest / len(pieces)))
        level = level * jnp.repeat(steps, shape[axis_at] // blocks).reshape([-1 if axis == axis_at else 1 for axis in range(len(shape))])
    return level


def bell_draw(rng, shape, spread, bound, cuts=(), dtype=jnp.bfloat16):
    entries = jax.random.normal(rng, shape, jnp.float32) * spread
    if len(cuts) > 0:
        entries = block_levels(rng, shape, cuts, -0.22, 0.18) * entries
    return jnp.clip(entries, min=-bound, max=bound).astype(dtype)


def setup_inputs(seed: int = 0) -> dict:
    splits = jax.random.split(jax.random.key(seed), 5)
    return {
        "forcing": bell_draw(splits[0], (FIELDS, GRID_X, GRID_Y, GRID_Z), 1.0, 6.0, ((2, 32), (3, 4)), jnp.float32),
        "symbol_x": jnp.clip(jax.random.uniform(splits[1], (GRID_X,), jnp.float32, 0.3, 3.0), 0.3, 3.0),
        "symbol_y": jnp.clip(jax.random.uniform(splits[2], (GRID_Y,), jnp.float32, 0.3, 3.0), 0.3, 3.0),
        "symbol_z": jnp.clip(jax.random.uniform(splits[3], (GRID_Z,), jnp.float32, 0.3, 3.0), 0.3, 3.0),
    }


def transform_table(count):
    rank = jnp.arange(count)
    angle = (jnp.pi / (4 * count)) * (((2 * rank[:, None] + 1) * (2 * rank[None, :] + 1)) % (8 * count)).astype(jnp.float32)
    return jnp.cos(angle) * (2.0 / count) ** 0.5


def to_modes(values, dim):
    moved = jnp.tensordot(values, transform_table(values.shape[dim]), axes=([dim], [0]), precision=lax.Precision.HIGHEST)
    return jnp.moveaxis(moved, -1, dim)


def reference(forcing, symbol_x, symbol_y, symbol_z):
    coefficients = forcing
    coefficients = to_modes(coefficients, 1)
    coefficients = to_modes(coefficients, 2)
    coefficients = to_modes(coefficients, 3)
    symbol = symbol_x[:, None, None] + symbol_y[None, :, None] + symbol_z[None, None, :]
    coefficients = coefficients * ((1.0 - 0.2 * symbol) / (1.0 + 0.2 * symbol))
    return coefficients
```

```python
import functools

import jax
import jax.numpy as jnp
import ml_dtypes
import numpy as np
from jax import lax
from jax.experimental import pallas as pl
from jax.experimental.pallas import tpu as pltpu
from jax.sharding import PartitionSpec as P

MESH = pl.DeviceIdType.MESH
F32, BF16 = jnp.float32, jnp.bfloat16
SIDE = 4
PLANE = SIDE * SIDE
STEPS = ((1, 0), (0, 1), (3, 0), (0, 3), (1, 1), (3, 3), (1, 3), (3, 1), (2, 0), (0, 2), (2, 1), (1, 2), (2, 3), (3, 2), (2, 2))
PIECES = 4


def table(count):
    rank = np.arange(count, dtype=np.int64)
    turns = ((2 * rank[:, None] + 1) * (2 * rank[None, :] + 1)) % (8 * count)
    exact = np.cos(np.pi / (4 * count) * turns) * np.sqrt(2.0 / count)
    high = exact.astype(np.float32).astype(ml_dtypes.bfloat16)
    low = (exact - high.astype(np.float64)).astype(np.float32).astype(ml_dtypes.bfloat16)
    return np.stack([high, low])


def split(value):
    high = value.astype(BF16)
    return high, (value - high.astype(F32)).astype(BF16)


def dot(a, b, b_dim=0):
    return lax.dot_general(a, b, (((1,), (b_dim,)), ((), ())), preferred_element_type=F32)


def kernel(
    x_hbm, sx_hbm, sy_hbm, sz_hbm, h_hbm, hz_hbm, o_hbm,
    xin, h, hz, xo, zr, yr, yo, pr, out, sx, sy, sz, sycol,
    in_sem, tab_sem, sym_sem, z_send, z_recv, xy_send, xy_recv, p_send, p_recv, o_sem,
):
    n = lax.axis_index("north")
    d = lax.axis_index("deep")
    half, q = n // PLANE, n % PLANE
    qx, qy = q % SIDE, q // SIDE
    group = 16 // PIECES

    table_copies = [
        pltpu.make_async_copy(h_hbm, h, tab_sem.at[0]),
        pltpu.make_async_copy(hz_hbm, hz, tab_sem.at[1]),
    ]
    table_copies[0].start()

    def in_copy(g, f):
        return pltpu.make_async_copy(
            x_hbm.at[f, pl.ds(g * group, group)], xin.at[pl.ds(g * group, group), f], in_sem.at[g, f]
        )

    for g in range(PIECES):
        for f in range(2):
            in_copy(g, f).start()
    table_copies[1].start()
    symbol_copies = [
        pltpu.make_async_copy(sx_hbm, sx, sym_sem.at[0]),
        pltpu.make_async_copy(sy_hbm, sy, sym_sem.at[1]),
        pltpu.make_async_copy(sz_hbm, sz, sym_sem.at[2]),
    ]
    for copy in symbol_copies:
        copy.start()

    def plane_chip(step):
        return ((qy + step[1]) % SIDE) * SIDE + (qx + step[0]) % SIDE

    across = ((1 - half) * PLANE + q, d)
    barrier = pltpu.get_barrier_semaphore()
    for step in STEPS:
        pl.semaphore_signal(barrier, inc=1, device_id=(half * PLANE + plane_chip(step), d), device_id_type=MESH)
    pl.semaphore_signal(barrier, inc=1, device_id=across, device_id_type=MESH)
    for flip in (1, 2, 3):
        pl.semaphore_signal(barrier, inc=1, device_id=(n, d ^ flip), device_id_type=MESH)
    pl.semaphore_wait(barrier, len(STEPS) + 4)

    def z_copy(c, g):
        return pltpu.make_async_remote_copy(
            src_ref=xo.at[1, c, :, pl.ds(g * group, group)],
            dst_ref=zr.at[c, :, pl.ds(g * group, group)],
            send_sem=z_send,
            recv_sem=z_recv.at[c, g],
            device_id=across,
            device_id_type=MESH,
        )

    table_copies[0].wait()

    def x_pair(i, carry):
        value = xin[pl.ds(2 * i, 2)].reshape(256, 512)
        high, low = split(value)
        for rel in (1, 0):
            side = jnp.where(rel == 1, 1 - half, half)
            rows = pl.ds(pl.multiple_of(side * 256, 256), 256)
            a_high, a_low = h[0, rows, :], h[1, rows, :]
            res = dot(a_high, high, 1) + dot(a_low, high, 1) + dot(a_high, low, 1)
            res = res.reshape(PLANE, 2, 8, 256)
            for c in range(2):
                for y in range(2):
                    xo[rel, c, :, 2 * i + y] = res[:, c, :, 128 * y : 128 * (y + 1)]
        return carry

    for g in range(PIECES):
        for f in range(2):
            in_copy(g, f).wait()
        lax.fori_loop(g * group // 2, (g + 1) * group // 2, x_pair, 0)
        z_copy(0, g).start()
    for g in range(PIECES):
        z_copy(1, g).start()

    def xy_own(c):
        for step in STEPS:
            to = plane_chip(step)
            pltpu.make_async_remote_copy(
                src_ref=xo.at[0, c, to],
                dst_ref=yr.at[c, n],
                send_sem=xy_send,
                recv_sem=xy_recv.at[c],
                device_id=(half * PLANE + to, d),
                device_id_type=MESH,
            ).start()
        yr[c, n] = xo[0, c, q]

    from_across = (1 - half) * PLANE + q

    def xy_relay(c):
        def piece(g, carry):
            z_copy(c, g).wait_recv()
            part = pl.ds(g * group, group)
            for step in STEPS:
                to = plane_chip(step)
                pltpu.make_async_remote_copy(
                    src_ref=zr.at[c, to, part],
                    dst_ref=yr.at[c, from_across, part],
                    send_sem=xy_send,
                    recv_sem=xy_recv.at[c],
                    device_id=(half * PLANE + to, d),
                    device_id_type=MESH,
                ).start()
            return carry

        lax.fori_loop(0, PIECES, piece, 0)
        yr[c, from_across] = zr[c, q]

    def along_y(c):
        pltpu.make_async_remote_copy(
            src_ref=yr.at[c, pl.ds(0, 30)],
            dst_ref=yr.at[c, pl.ds(0, 30)],
            send_sem=xy_send,
            recv_sem=xy_recv.at[c],
            device_id=across,
            device_id_type=MESH,
        ).wait_recv()
        lines = yr.at[c].reshape(4096, 128)

        def pair(i, carry):
            value = jnp.concatenate([lines[pl.ds(2 * i + k, 512, stride=8), :] for k in range(2)], axis=1)
            high, low = split(value)
            for part in range(2):
                rows = pl.ds(part * 256, 256)
                a_high, a_low = h[0, rows, :], h[1, rows, :]
                res = dot(a_high, high) + dot(a_low, high) + dot(a_high, low)
                for k in range(2):
                    for s in range(2):
                        yo[c, 2 * part + s, 2 * i + k] = res[128 * s : 128 * (s + 1), 128 * k : 128 * (k + 1)]
            for k in range(2):
                pr[c, d, 2 * i + k] = yo[c, d, 2 * i + k]
                for flip in (2, 3, 1):
                    pltpu.make_async_remote_copy(
                        src_ref=yo.at[c, d ^ flip, 2 * i + k],
                        dst_ref=pr.at[c, d, 2 * i + k],
                        send_sem=p_send,
                        recv_sem=p_recv.at[c, 2 * i + k],
                        device_id=(n, d ^ flip),
                        device_id_type=MESH,
                    ).start()
            return carry

        lax.fori_loop(0, 4, pair, 0)

    def along_z(c):
        first = lax.broadcasted_iota(jnp.int32, (128, 128), 1) < 64

        def line(j, carry):
            pltpu.make_async_remote_copy(
                src_ref=pr.at[c, pl.ds(0, 3), 0],
                dst_ref=pr.at[c, pl.ds(0, 3), 0],
                send_sem=p_send,
                recv_sem=p_recv.at[c, j],
                device_id=across,
                device_id_type=MESH,
            ).wait_recv()
            parts = [pr[c, s, j] for s in range(4)]
            turned = [pltpu.roll(p, 64, 1) for p in parts]
            field = [
                jnp.concatenate([jnp.where(first, parts[s], turned[s + 1]) for s in (0, 2)], axis=1),
                jnp.concatenate([jnp.where(first, turned[s], parts[s + 1]) for s in (0, 2)], axis=1),
            ]
            high, low = split(jnp.concatenate(field, axis=0))
            res = dot(high, hz[0]) + dot(high, hz[1]) + dot(low, hz[0])
            symbol = (sx[n * 16 + c * 8 + j] + sycol[...]) + sz[...]
            factor = (1.0 - 0.2 * symbol) / (1.0 + 0.2 * symbol)
            for f in range(2):
                out[f, c * 8 + j] = res[128 * f : 128 * (f + 1)] * factor
            pltpu.make_async_copy(out.at[:, c * 8 + j], o_hbm.at[:, c * 8 + j], o_sem).start()
            return carry

        lax.fori_loop(0, 8, line, 0)

    xy_own(0)
    xy_relay(0)
    xy_own(1)
    for copy in symbol_copies:
        copy.wait()
    table_copies[1].wait()
    along = sy[pl.ds(d, 1), :]
    sycol[...] = jnp.concatenate([jnp.transpose(jnp.broadcast_to(along, (128, 128)))] * 2, axis=1)
    along_y(0)
    xy_relay(1)
    along_y(1)
    along_z(0)
    along_z(1)

    def drain(ref, sem):
        pltpu.make_async_remote_copy(
            src_ref=ref, dst_ref=ref, send_sem=sem, recv_sem=p_recv.at[0, 0], device_id=across, device_id_type=MESH
        ).wait_send()

    drain(zr, z_send)
    for c in range(2):
        drain(yr.at[c, pl.ds(0, 30)], xy_send)
        drain(pr.at[c, pl.ds(0, 3)], p_send)
    pltpu.make_async_copy(out, o_hbm, o_sem).wait()


def local(forcing, symbol_x, symbol_y, symbol_z):
    lines = jnp.transpose(forcing, (0, 2, 3, 1))
    return pl.pallas_call(
        kernel,
        out_shape=jax.ShapeDtypeStruct((2, 16, 128, 256), F32),
        in_specs=[pl.BlockSpec(memory_space=pl.ANY)] * 6,
        out_specs=pl.BlockSpec(memory_space=pl.ANY),
        scratch_shapes=[
            pltpu.VMEM((16, 2, 64, 512), F32),
            pltpu.VMEM((2, 512, 512), BF16),
            pltpu.VMEM((2, 256, 256), BF16),
            pltpu.VMEM((2, 2, 16, 16, 8, 128), F32),
            pltpu.VMEM((2, 16, 16, 8, 128), F32),
            pltpu.VMEM((2, 32, 16, 8, 128), F32),
            pltpu.VMEM((2, 4, 8, 128, 128), F32),
            pltpu.VMEM((2, 4, 8, 128, 128), F32),
            pltpu.VMEM((2, 16, 128, 256), F32),
            pltpu.SMEM((512,), F32),
            pltpu.VMEM((4, 128), F32),
            pltpu.VMEM((1, 256), F32),
            pltpu.VMEM((128, 256), F32),
            pltpu.SemaphoreType.DMA((PIECES, 2)),
            pltpu.SemaphoreType.DMA((2,)),
            pltpu.SemaphoreType.DMA((3,)),
            pltpu.SemaphoreType.DMA,
            pltpu.SemaphoreType.DMA((2, PIECES)),
            pltpu.SemaphoreType.DMA,
            pltpu.SemaphoreType.DMA((2,)),
            pltpu.SemaphoreType.DMA,
            pltpu.SemaphoreType.DMA((2, 8)),
            pltpu.SemaphoreType.DMA,
        ],
        compiler_params=pltpu.CompilerParams(
            collective_id=0, has_side_effects=True, vmem_limit_bytes=48 * 2**20
        ),
        name="transform",
    )(
        lines, symbol_x, symbol_y.reshape(4, 128), symbol_z.reshape(1, 256),
        jnp.asarray(table(512)), jnp.asarray(table(256)),
    )


def solution(mesh):
    return jax.shard_map(
        local,
        mesh=mesh,
        in_specs=(P(None, None, "north", "deep"), P(), P(), P()),
        out_specs=P(None, "north", "deep", None),
        check_vma=False,
    )
```

```python
import functools

import jax
import jax.numpy as jnp
import ml_dtypes
import numpy as np
from jax import lax
from jax.experimental import pallas as pl
from jax.experimental.pallas import tpu as pltpu
from jax.sharding import PartitionSpec as P

MESH = pl.DeviceIdType.MESH
F32, BF16 = jnp.float32, jnp.bfloat16
SIDE = 4
PLANE = SIDE * SIDE
STEPS = ((1, 0), (0, 1), (3, 0), (0, 3), (1, 1), (3, 3), (1, 3), (3, 1), (2, 0), (0, 2), (2, 1), (1, 2), (2, 3), (3, 2), (2, 2))
LINE = tuple(step for step in STEPS if 0 in step)
PIECES = 4


def table(count):
    rank = np.arange(count, dtype=np.int64)
    turns = ((2 * rank[:, None] + 1) * (2 * rank[None, :] + 1)) % (8 * count)
    exact = np.cos(np.pi / (4 * count) * turns) * np.sqrt(2.0 / count)
    high = exact.astype(np.float32).astype(ml_dtypes.bfloat16)
    low = (exact - high.astype(np.float64)).astype(np.float32).astype(ml_dtypes.bfloat16)
    return np.stack([high, low])


def split(value):
    high = value.astype(BF16)
    return high, (value - high.astype(F32)).astype(BF16)


def dot(a, b, b_dim=0):
    return lax.dot_general(a, b, (((1,), (b_dim,)), ((), ())), preferred_element_type=F32)


def kernel(
    x_hbm, sx_hbm, sy_hbm, sz_hbm, h_hbm, hz_hbm, out,
    xin, h, hz, xo, zr, yr, yo, pr, sx, sy, sz, sycol,
    in_sem, tab_sem, sym_sem, z_send, z_recv, xy_send, xy_recv, p_send, p_recv, ready,
):
    n = lax.axis_index("north")
    d = lax.axis_index("deep")
    half, q = n // PLANE, n % PLANE
    qx, qy = q % SIDE, q // SIDE
    group = 16 // PIECES

    table_copies = [
        pltpu.make_async_copy(h_hbm, h, tab_sem.at[0]),
        pltpu.make_async_copy(hz_hbm, hz, tab_sem.at[1]),
    ]
    table_copies[0].start()

    def in_copy(i, f):
        return pltpu.make_async_copy(x_hbm.at[f, pl.ds(2 * i, 2)], xin.at[pl.ds(2 * i, 2), f], in_sem.at[i, f])

    for i in range(8):
        for f in range(2):
            in_copy(i, f).start()
    table_copies[1].start()
    symbol_copies = [
        pltpu.make_async_copy(sx_hbm, sx, sym_sem.at[0]),
        pltpu.make_async_copy(sy_hbm, sy, sym_sem.at[1]),
        pltpu.make_async_copy(sz_hbm, sz, sym_sem.at[2]),
    ]
    for copy in symbol_copies:
        copy.start()

    def plane_chip(step):
        return ((qy + step[1]) % SIDE) * SIDE + (qx + step[0]) % SIDE

    across = ((1 - half) * PLANE + q, d)
    barrier = pltpu.get_barrier_semaphore()
    pl.semaphore_signal(barrier, inc=1, device_id=across, device_id_type=MESH)
    for step in LINE:
        pl.semaphore_signal(barrier, inc=1, device_id=(half * PLANE + plane_chip(step), d), device_id_type=MESH)
    for flip in (1, 2, 3):
        pl.semaphore_signal(barrier, inc=1, device_id=(n, d ^ flip), device_id_type=MESH)

    def z_copy(c, i, count):
        part = pl.ds(i, count)
        return pltpu.make_async_remote_copy(
            src_ref=xo.at[1, c, :, part],
            dst_ref=zr.at[c, :, part],
            send_sem=z_send,
            recv_sem=z_recv.at[c, i // group],
            device_id=across,
            device_id_type=MESH,
        )

    table_copies[0].wait()

    def x_pair(i, carry):
        value = xin[pl.ds(2 * i, 2)].reshape(256, 512)
        high, low = split(value)
        for rel in (1, 0):
            side = jnp.where(rel == 1, 1 - half, half)
            rows = pl.ds(pl.multiple_of(side * 256, 256), 256)
            a_high, a_low = h[0, rows, :], h[1, rows, :]
            res = dot(a_high, high, 1) + dot(a_low, high, 1) + dot(a_high, low, 1)
            res = res.reshape(PLANE, 2, 8, 256)
            for c in range(2):
                for y in range(2):
                    xo[rel, c, :, 2 * i + y] = res[:, c, :, 128 * y : 128 * (y + 1)]
        return carry

    def x_step(i, carry):
        for f in range(2):
            in_copy(i, f).wait()
        x_pair(i, carry)
        z_copy(0, 2 * i, 2).start()
        return carry

    for f in range(2):
        in_copy(0, f).wait()
    x_pair(0, 0)
    pl.semaphore_wait(barrier, len(LINE) + 4)
    z_copy(0, 0, 2).start()
    for step in LINE:
        if step[1] == 0:
            pl.semaphore_signal(ready, inc=1, device_id=(half * PLANE + plane_chip(step), d), device_id_type=MESH)
    lax.fori_loop(1, 8, x_step, 0)
    for g in range(PIECES):
        z_copy(1, g * group, group).start()
    pl.semaphore_wait(ready, SIDE - 1)

    def xy_own(c):
        for step in STEPS:
            to = plane_chip(step)
            pltpu.make_async_remote_copy(
                src_ref=xo.at[0, c, to],
                dst_ref=yr.at[c, n],
                send_sem=xy_send,
                recv_sem=xy_recv.at[c],
                device_id=(half * PLANE + to, d),
                device_id_type=MESH,
            ).start()
        yr[c, n] = xo[0, c, q]

    from_across = (1 - half) * PLANE + q

    def xy_relay(c):
        def piece(g, carry):
            z_copy(c, g * group, group).wait_recv()
            part = pl.ds(g * group, group)
            for step in STEPS:
                to = plane_chip(step)
                pltpu.make_async_remote_copy(
                    src_ref=zr.at[c, to, part],
                    dst_ref=yr.at[c, from_across, part],
                    send_sem=xy_send,
                    recv_sem=xy_recv.at[c],
                    device_id=(half * PLANE + to, d),
                    device_id_type=MESH,
                ).start()
            return carry

        lax.fori_loop(0, PIECES, piece, 0)
        yr[c, from_across] = zr[c, q]

    def along_y(c):
        pltpu.make_async_remote_copy(
            src_ref=yr.at[c, pl.ds(0, 30)],
            dst_ref=yr.at[c, pl.ds(0, 30)],
            send_sem=xy_send,
            recv_sem=xy_recv.at[c],
            device_id=across,
            device_id_type=MESH,
        ).wait_recv()
        lines = yr.at[c].reshape(4096, 128)

        def pair(i, carry):
            value = jnp.concatenate([lines[pl.ds(2 * i + k, 512, stride=8), :] for k in range(2)], axis=1)
            high, low = split(value)
            for part in range(2):
                rows = pl.ds(part * 256, 256)
                a_high, a_low = h[0, rows, :], h[1, rows, :]
                res = dot(a_high, high) + dot(a_low, high) + dot(a_high, low)
                for k in range(2):
                    for s in range(2):
                        yo[c, 2 * part + s, 2 * i + k] = res[128 * s : 128 * (s + 1), 128 * k : 128 * (k + 1)]
            for k in range(2):
                pr[c, d, 2 * i + k] = yo[c, d, 2 * i + k]
                for flip in (2, 3, 1):
                    pltpu.make_async_remote_copy(
                        src_ref=yo.at[c, d ^ flip, 2 * i + k],
                        dst_ref=pr.at[c, d, 2 * i + k],
                        send_sem=p_send,
                        recv_sem=p_recv.at[c, 2 * i + k],
                        device_id=(n, d ^ flip),
                        device_id_type=MESH,
                    ).start()
            return carry

        lax.fori_loop(0, 4, pair, 0)

    def along_z(c):
        first = lax.broadcasted_iota(jnp.int32, (128, 128), 1) < 64

        def line(j, carry):
            pltpu.make_async_remote_copy(
                src_ref=pr.at[c, pl.ds(0, 3), 0],
                dst_ref=pr.at[c, pl.ds(0, 3), 0],
                send_sem=p_send,
                recv_sem=p_recv.at[c, j],
                device_id=across,
                device_id_type=MESH,
            ).wait_recv()
            parts = [pr[c, s, j] for s in range(4)]
            turned = [pltpu.roll(p, 64, 1) for p in parts]
            field = [
                jnp.concatenate([jnp.where(first, parts[s], turned[s + 1]) for s in (0, 2)], axis=1),
                jnp.concatenate([jnp.where(first, turned[s], parts[s + 1]) for s in (0, 2)], axis=1),
            ]
            high, low = split(jnp.concatenate(field, axis=0))
            res = dot(high, hz[0]) + dot(high, hz[1]) + dot(low, hz[0])
            symbol = (sx[n * 16 + c * 8 + j] + sycol[...]) + sz[...]
            factor = (1.0 - 0.2 * symbol) / (1.0 + 0.2 * symbol)
            for f in range(2):
                out[f, c * 8 + j] = res[128 * f : 128 * (f + 1)] * factor
            return carry

        lax.fori_loop(0, 8, line, 0)

    xy_own(0)
    xy_relay(0)
    xy_own(1)
    for copy in symbol_copies:
        copy.wait()
    table_copies[1].wait()
    along = sy[pl.ds(d, 1), :]
    sycol[...] = jnp.concatenate([jnp.transpose(jnp.broadcast_to(along, (128, 128)))] * 2, axis=1)
    along_y(0)
    xy_relay(1)
    along_y(1)
    along_z(0)
    along_z(1)

    def drain(ref, sem):
        pltpu.make_async_remote_copy(
            src_ref=ref, dst_ref=ref, send_sem=sem, recv_sem=p_recv.at[0, 0], device_id=across, device_id_type=MESH
        ).wait_send()

    drain(zr, z_send)
    for c in range(2):
        drain(yr.at[c, pl.ds(0, 30)], xy_send)
        drain(pr.at[c, pl.ds(0, 3)], p_send)


def local(forcing, symbol_x, symbol_y, symbol_z):
    lines = jnp.transpose(forcing, (0, 2, 3, 1))
    return pl.pallas_call(
        kernel,
        out_shape=jax.ShapeDtypeStruct((2, 16, 128, 256), F32),
        in_specs=[pl.BlockSpec(memory_space=pltpu.HBM)] * 6,
        out_specs=pl.BlockSpec(memory_space=pltpu.VMEM),
        scratch_shapes=[
            pltpu.VMEM((16, 2, 64, 512), F32),
            pltpu.VMEM((2, 512, 512), BF16),
            pltpu.VMEM((2, 256, 256), BF16),
            pltpu.VMEM((2, 2, 16, 16, 8, 128), F32),
            pltpu.VMEM((2, 16, 16, 8, 128), F32),
            pltpu.VMEM((2, 32, 16, 8, 128), F32),
            pltpu.VMEM((2, 4, 8, 128, 128), F32),
            pltpu.VMEM((2, 4, 8, 128, 128), F32),
            pltpu.SMEM((512,), F32),
            pltpu.VMEM((4, 128), F32),
            pltpu.VMEM((1, 256), F32),
            pltpu.VMEM((128, 256), F32),
            pltpu.SemaphoreType.DMA((8, 2)),
            pltpu.SemaphoreType.DMA((2,)),
            pltpu.SemaphoreType.DMA((3,)),
            pltpu.SemaphoreType.DMA,
            pltpu.SemaphoreType.DMA((2, PIECES)),
            pltpu.SemaphoreType.DMA,
            pltpu.SemaphoreType.DMA((2,)),
            pltpu.SemaphoreType.DMA,
            pltpu.SemaphoreType.DMA((2, 8)),
            pltpu.SemaphoreType.REGULAR,
        ],
        compiler_params=pltpu.CompilerParams(
            collective_id=0, has_side_effects=True, vmem_limit_bytes=48 * 2**20
        ),
        name="transform",
    )(
        *(
            pltpu.with_memory_space_constraint(value, pltpu.HBM)
            for value in (
                lines,
                symbol_x,
                symbol_y.reshape(4, 128),
                symbol_z.reshape(1, 256),
                jnp.asarray(table(512)),
                jnp.asarray(table(256)),
            )
        )
    )


def solution(mesh):
    return jax.shard_map(
        local,
        mesh=mesh,
        in_specs=(P(None, None, "north", "deep"), P(), P(), P()),
        out_specs=P(None, "north", "deep", None),
        check_vma=False,
    )
```

```python
import functools

import jax
import jax.numpy as jnp
import ml_dtypes
import numpy as np
from jax import lax
from jax.experimental import pallas as pl
from jax.experimental.pallas import tpu as pltpu
from jax.sharding import PartitionSpec as P

MESH = pl.DeviceIdType.MESH
F32, BF16 = jnp.float32, jnp.bfloat16
SIDE = 4
PLANE = SIDE * SIDE
STEPS = ((1, 0), (0, 1), (3, 0), (0, 3), (1, 1), (3, 3), (1, 3), (3, 1), (2, 0), (0, 2), (2, 1), (1, 2), (2, 3), (3, 2), (2, 2))
LINE = tuple(step for step in STEPS if 0 in step)
PIECES = 4

LINES = (2, 1)


def table(count):
    rank = np.arange(count, dtype=np.int64)
    turns = ((2 * rank[:, None] + 1) * (2 * rank[None, :] + 1)) % (8 * count)
    exact = np.cos(np.pi / (4 * count) * turns) * np.sqrt(2.0 / count)
    high = exact.astype(np.float32).astype(ml_dtypes.bfloat16)
    low = (exact - high.astype(np.float64)).astype(np.float32).astype(ml_dtypes.bfloat16)
    return np.stack([high, low])


def split(value):
    high = value.astype(BF16)
    return high, (value - high.astype(F32)).astype(BF16)


def dot(a, b, b_dim=0):
    return lax.dot_general(a, b, (((1,), (b_dim,)), ((), ())), preferred_element_type=F32)


def kernel(
    x_hbm, sx_hbm, sy_hbm, sz_hbm, h_hbm, hz_hbm, out,
    xin, h, hz, xo, zr, yr, yo, pr, fw, via, sx, sy, sz, sycol, factor,
    in_sem, tab_sem, sym_sem, z_send, z_recv, xy_send, xy_recv, p_send, p_recv, f_send, f_recv, v_sem, near, far, row, column,
):
    n = lax.axis_index("north")
    d = lax.axis_index("deep")
    half, q = n // PLANE, n % PLANE
    qx, qy = q % SIDE, q // SIDE
    group = 16 // PIECES

    def table_copy(rel):
        side = jnp.where(rel == 1, 1 - half, half)
        rows = pl.ds(pl.multiple_of(side * 256, 256), 256)
        return pltpu.make_async_copy(h_hbm.at[:, rows], h.at[:, rows], tab_sem.at[rel])

    hz_copy = pltpu.make_async_copy(hz_hbm, hz, tab_sem.at[2])
    table_copy(1).start()

    def in_copy(i, f):
        return pltpu.make_async_copy(x_hbm.at[f, pl.ds(2 * i, 2)], xin.at[pl.ds(2 * i, 2), f], in_sem.at[min(i, 1)])

    for f in range(2):
        in_copy(0, f).start()
    symbol_copies = [
        pltpu.make_async_copy(sx_hbm, sx, sym_sem.at[0]),
        pltpu.make_async_copy(sy_hbm, sy, sym_sem.at[1]),
        pltpu.make_async_copy(sz_hbm, sz, sym_sem.at[2]),
    ]

    def plane_chip(step):
        return ((qy + step[1]) % SIDE) * SIDE + (qx + step[0]) % SIDE

    across = ((1 - half) * PLANE + q, d)
    mate, twin, beyond = (n, d ^ 2), (n, d ^ 1), ((1 - half) * PLANE + q, d ^ 2)
    middle = half != d // 2
    outer = half == d // 2

    def tell(semaphore, to):
        pl.semaphore_signal(semaphore, inc=1, device_id=to, device_id_type=MESH)

    barrier = pltpu.get_barrier_semaphore()
    for peer in (mate, twin):
        tell(barrier, peer)
    pl.when(middle)(lambda: tell(barrier, beyond))
    pl.when(qx > 0)(lambda: tell(barrier, (n - 1, d)))
    pl.when(qx < SIDE - 1)(lambda: tell(barrier, (n + 1, d)))
    pl.when(qy > 0)(lambda: tell(barrier, (n - SIDE, d)))
    pl.when(qy < SIDE - 1)(lambda: tell(barrier, (n + SIDE, d)))
    contacts = 2 + middle.astype(jnp.int32)
    for at in (qx, qy):
        contacts += (at > 0).astype(jnp.int32) + (at < SIDE - 1).astype(jnp.int32)

    def sweep(sems, at, stride):
        pl.when(at > 0)(lambda: pl.semaphore_wait(sems.at[0], 1))
        pl.when(at < SIDE - 1)(lambda: tell(sems.at[0], (n + stride, d)))
        pl.when(at < SIDE - 1)(lambda: pl.semaphore_wait(sems.at[1], 1))
        pl.when(at > 0)(lambda: tell(sems.at[1], (n - stride, d)))

    def z_copy(c, i, count):
        part = pl.ds(i, count)
        return pltpu.make_async_remote_copy(
            src_ref=xo.at[1, c, :, part],
            dst_ref=zr.at[c, :, part],
            send_sem=z_send,
            recv_sem=z_recv.at[c, i // group],
            device_id=across,
            device_id_type=MESH,
        )


    def x_half(i, rel):
        value = xin[pl.ds(2 * i, 2)].reshape(256, 512)
        high, low = split(value)
        side = jnp.where(rel == 1, 1 - half, half)
        rows = pl.ds(pl.multiple_of(side * 256, 256), 256)
        a_high, a_low = h[0, rows, :], h[1, rows, :]
        res = dot(a_high, high, 1) + dot(a_low, high, 1) + dot(a_high, low, 1)
        res = res.reshape(PLANE, 2, 8, 256)
        for c in range(2):
            for y in range(2):
                xo[rel, c, :, 2 * i + y] = res[:, c, :, 128 * y : 128 * (y + 1)]

    def x_pair(i):
        high, low = split(xin[pl.ds(2 * i, 2)].reshape(256, 512))
        for rel in (1, 0):
            side = jnp.where(rel == 1, 1 - half, half)
            rows = pl.ds(pl.multiple_of(side * 256, 256), 256)
            a_high, a_low = h[0, rows, :], h[1, rows, :]
            res = dot(a_high, high, 1) + dot(a_low, high, 1) + dot(a_high, low, 1)
            res = res.reshape(PLANE, 2, 8, 256)
            for c in range(2):
                for y in range(2):
                    xo[rel, c, :, 2 * i + y] = res[:, c, :, 128 * y : 128 * (y + 1)]

    def x_step(i, carry):
        x_pair(i)
        z_copy(0, 2 * i, 2).start()
        return carry

    first_copy = pltpu.make_async_remote_copy(
        src_ref=xo.at[1, 1, :, pl.ds(0, 2)],
        dst_ref=via,
        send_sem=v_sem.at[0],
        recv_sem=v_sem.at[1],
        device_id=mate,
        device_id_type=MESH,
    )
    onward_copy = pltpu.make_async_remote_copy(
        src_ref=via,
        dst_ref=zr.at[1, :, pl.ds(0, 2)],
        send_sem=z_send,
        recv_sem=z_recv.at[1, 0],
        device_id=beyond,
        device_id_type=MESH,
    )
    def in_wait(planes, k):
        pltpu.make_async_copy(xin.at[planes], xin.at[planes], in_sem.at[k]).wait()

    table_copy(1).wait()
    in_wait(pl.ds(0, 2), 0)
    table_copy(0).start()
    for i in range(1, 8):
        for f in range(2):
            in_copy(i, f).start()
    for copy in [hz_copy, *symbol_copies]:
        copy.start()
    x_half(0, 1)
    pl.semaphore_wait(barrier, contacts)
    first_copy.start()
    @pl.when(middle)
    def _():
        tell(near, mate)
        tell(near, beyond)

    table_copy(0).wait()
    x_half(0, 0)
    pl.semaphore_wait(near, 1)
    z_copy(0, 0, 2).start()
    pl.when(middle)(lambda: tell(far, across))
    in_wait(pl.ds(2, 14), 1)
    lax.fori_loop(1, 4, x_step, 0)
    sweep(row, qx, 1)
    lax.fori_loop(4, 7, x_step, 0)
    sweep(column, qy, SIDE)
    x_step(7, 0)
    first_copy.wait_recv()
    pl.when(outer)(lambda: pl.semaphore_wait(far, 1))
    onward_copy.start()
    z_copy(1, 2, 2).start()
    for g in range(1, PIECES):
        z_copy(1, g * group, group).start()

    def xy_own(c):
        for step in STEPS:
            to = plane_chip(step)
            pltpu.make_async_remote_copy(
                src_ref=xo.at[0, c, to],
                dst_ref=yr.at[c, n],
                send_sem=xy_send,
                recv_sem=xy_recv.at[c],
                device_id=(half * PLANE + to, d),
                device_id_type=MESH,
            ).start()
        yr[c, n] = xo[0, c, q]

    from_across = (1 - half) * PLANE + q

    def xy_relay(c):
        def piece(k, carry):
            g = (k + c) % PIECES
            z_copy(c, g * group, group).wait_recv()
            part = pl.ds(g * group, group)
            for step in STEPS:
                to = plane_chip(step)
                pltpu.make_async_remote_copy(
                    src_ref=zr.at[c, to, part],
                    dst_ref=yr.at[c, from_across, part],
                    send_sem=xy_send,
                    recv_sem=xy_recv.at[c],
                    device_id=(half * PLANE + to, d),
                    device_id_type=MESH,
                ).start()
            return carry

        lax.fori_loop(0, PIECES, piece, 0)
        yr[c, from_across] = zr[c, q]

    def firsts(c):
        return range(0, 2, LINES[c])

    def p_copy(ref, source, c, j, to):
        part = pl.ds(j, LINES[c])
        return pltpu.make_async_remote_copy(
            src_ref=ref.at[part],
            dst_ref=pr.at[c, source, part],
            send_sem=p_send,
            recv_sem=p_recv.at[c * 4 + j // LINES[c]],
            device_id=(n, to),
            device_id_type=MESH,
        )

    def to_twin(c, i):
        part = pl.ds(2 * i, 2)
        return pltpu.make_async_remote_copy(
            src_ref=yo.at[c, d ^ 3, part],
            dst_ref=fw.at[c, part],
            send_sem=f_send,
            recv_sem=f_recv.at[c * 4 + i],
            device_id=(n, d ^ 1),
            device_id_type=MESH,
        )

    def onward(c, i):
        to_twin(c, i).wait_recv()
        for j in firsts(c):
            p_copy(fw.at[c], d ^ 1, c, 2 * i + j, d ^ 2).start()

    def along_y(c):
        pltpu.make_async_remote_copy(
            src_ref=yr.at[c, pl.ds(0, 30)],
            dst_ref=yr.at[c, pl.ds(0, 30)],
            send_sem=xy_send,
            recv_sem=xy_recv.at[c],
            device_id=across,
            device_id_type=MESH,
        ).wait_recv()
        lines = yr.at[c].reshape(4096, 128)

        def pair(i, carry):
            value = jnp.concatenate([lines[pl.ds(2 * i + k, 512, stride=8), :] for k in range(2)], axis=1)
            high, low = split(value)
            for part in range(2):
                rows = pl.ds(part * 256, 256)
                a_high, a_low = h[0, rows, :], h[1, rows, :]
                res = dot(a_high, high) + dot(a_low, high) + dot(a_high, low)
                for k in range(2):
                    for s in range(2):
                        yo[c, 2 * part + s, 2 * i + k] = res[128 * s : 128 * (s + 1), 128 * k : 128 * (k + 1)]
            pr[c, d, pl.ds(2 * i, 2)] = yo[c, d, pl.ds(2 * i, 2)]
            to_twin(c, i).start()
            for j in firsts(c):
                p_copy(yo.at[c, d ^ 1], d, c, 2 * i + j, d ^ 1).start()
                p_copy(yo.at[c, d ^ 2], d, c, 2 * i + j, d ^ 2).start()

            @pl.when(i > 0)
            def _():
                onward(c, i - 1)

            return carry

        lax.fori_loop(0, 4, pair, 0)
        onward(c, 3)

    def along_z(c):
        first = lax.broadcasted_iota(jnp.int32, (128, 128), 1) < 64

        def line(j, carry):
            symbol = (sx[n * 16 + c * 8 + j] + sycol[...]) + sz[...]
            factor[...] = (1.0 - 0.2 * symbol) / (1.0 + 0.2 * symbol)

            @pl.when(j % LINES[c] == 0)
            def _():
                whole = pr.at[c, pl.ds(0, 3), pl.ds(0, LINES[c])]
                pltpu.make_async_remote_copy(
                    src_ref=whole,
                    dst_ref=whole,
                    send_sem=p_send,
                    recv_sem=p_recv.at[c * 4 + j // LINES[c]],
                    device_id=across,
                    device_id_type=MESH,
                ).wait_recv()

            parts = [pr[c, s, j] for s in range(4)]
            turned = [pltpu.roll(p, 64, 1) for p in parts]
            field = [
                jnp.concatenate([jnp.where(first, parts[s], turned[s + 1]) for s in (0, 2)], axis=1),
                jnp.concatenate([jnp.where(first, turned[s], parts[s + 1]) for s in (0, 2)], axis=1),
            ]
            high, low = split(jnp.concatenate(field, axis=0))
            res = dot(high, hz[0]) + dot(high, hz[1]) + dot(low, hz[0])
            for f in range(2):
                out[f, c * 8 + j] = res[128 * f : 128 * (f + 1)] * factor[...]
            return carry

        lax.fori_loop(0, 8, line, 0)

    xy_own(0)
    xy_relay(0)
    xy_own(1)
    for copy in symbol_copies:
        copy.wait()
    hz_copy.wait()
    along = sy[pl.ds(d, 1), :]
    sycol[...] = jnp.concatenate([jnp.transpose(jnp.broadcast_to(along, (128, 128)))] * 2, axis=1)
    along_y(0)
    xy_relay(1)
    along_y(1)
    along_z(0)
    along_z(1)

    def drain(ref, sem):
        pltpu.make_async_remote_copy(
            src_ref=ref, dst_ref=ref, send_sem=sem, recv_sem=p_recv.at[0], device_id=across, device_id_type=MESH
        ).wait_send()

    first_copy.wait_send()
    drain(zr, z_send)
    for c in range(2):
        drain(yr.at[c, pl.ds(0, 30)], xy_send)
        drain(pr.at[c, pl.ds(0, 3)], p_send)
        drain(fw.at[c], f_send)


def local(forcing, symbol_x, symbol_y, symbol_z):
    lines = jnp.transpose(forcing, (0, 2, 3, 1))
    return pl.pallas_call(
        kernel,
        out_shape=jax.ShapeDtypeStruct((2, 16, 128, 256), F32),
        in_specs=[pl.BlockSpec(memory_space=pltpu.HBM)] * 6,
        out_specs=pl.BlockSpec(memory_space=pltpu.VMEM),
        scratch_shapes=[
            pltpu.VMEM((16, 2, 64, 512), F32),
            pltpu.VMEM((2, 512, 512), BF16),
            pltpu.VMEM((2, 256, 256), BF16),
            pltpu.VMEM((2, 2, 16, 16, 8, 128), F32),
            pltpu.VMEM((2, 16, 16, 8, 128), F32),
            pltpu.VMEM((2, 32, 16, 8, 128), F32),
            pltpu.VMEM((2, 4, 8, 128, 128), F32),
            pltpu.VMEM((2, 4, 8, 128, 128), F32),
            pltpu.VMEM((2, 8, 128, 128), F32),
            pltpu.VMEM((16, 2, 8, 128), F32),
            pltpu.SMEM((512,), F32),
            pltpu.VMEM((4, 128), F32),
            pltpu.VMEM((1, 256), F32),
            pltpu.VMEM((128, 256), F32),
            pltpu.VMEM((128, 256), F32),
            pltpu.SemaphoreType.DMA((2,)),
            pltpu.SemaphoreType.DMA((3,)),
            pltpu.SemaphoreType.DMA((3,)),
            pltpu.SemaphoreType.DMA,
            pltpu.SemaphoreType.DMA((2, PIECES)),
            pltpu.SemaphoreType.DMA,
            pltpu.SemaphoreType.DMA((2,)),
            pltpu.SemaphoreType.DMA,
            pltpu.SemaphoreType.DMA((12,)),
            pltpu.SemaphoreType.DMA,
            pltpu.SemaphoreType.DMA((8,)),
            pltpu.SemaphoreType.DMA((2,)),
            pltpu.SemaphoreType.REGULAR,
            pltpu.SemaphoreType.REGULAR,
            pltpu.SemaphoreType.REGULAR((2,)),
            pltpu.SemaphoreType.REGULAR((2,)),
        ],
        compiler_params=pltpu.CompilerParams(
            collective_id=0, has_side_effects=True, vmem_limit_bytes=48 * 2**20
        ),
        name="transform",
    )(
        *(
            pltpu.with_memory_space_constraint(value, pltpu.HBM)
            for value in (
                lines,
                symbol_x,
                symbol_y.reshape(4, 128),
                symbol_z.reshape(1, 256),
                jnp.asarray(table(512)),
                jnp.asarray(table(256)),
            )
        )
    )


def solution(mesh):
    return jax.shard_map(
        local,
        mesh=mesh,
        in_specs=(P(None, None, "north", "deep"), P(), P(), P()),
        out_specs=P(None, "north", "deep", None),
        check_vma=False,
    )
```

```python
import functools

import jax
import jax.numpy as jnp
import ml_dtypes
import numpy as np
from jax import lax
from jax.experimental import pallas as pl
from jax.experimental.pallas import tpu as pltpu
from jax.sharding import PartitionSpec as P

MESH = pl.DeviceIdType.MESH
F32, BF16 = jnp.float32, jnp.bfloat16
SIDE = 4
PLANE = SIDE * SIDE
STEPS = ((1, 0), (0, 1), (3, 0), (0, 3), (1, 1), (3, 3), (1, 3), (3, 1), (2, 0), (0, 2), (2, 1), (1, 2), (2, 3), (3, 2), (2, 2))
LINE = tuple(step for step in STEPS if 0 in step)
PIECES = 4

LINES = (2, 1)


def table(count):
    rank = np.arange(count, dtype=np.int64)
    turns = ((2 * rank[:, None] + 1) * (2 * rank[None, :] + 1)) % (8 * count)
    exact = np.cos(np.pi / (4 * count) * turns) * np.sqrt(2.0 / count)
    high = exact.astype(np.float32).astype(ml_dtypes.bfloat16)
    low = (exact - high.astype(np.float64)).astype(np.float32).astype(ml_dtypes.bfloat16)
    return np.stack([high, low])


def by_chunk(rows):
    parts = rows.reshape(2, 2, PLANE, 2, 8, rows.shape[-1])
    return np.ascontiguousarray(parts.transpose(0, 1, 3, 2, 4, 5)).reshape(rows.shape)


def split(value):
    high = value.astype(BF16)
    return high, (value - high.astype(F32)).astype(BF16)


def dot(a, b, b_dim=0):
    return lax.dot_general(a, b, (((1,), (b_dim,)), ((), ())), preferred_element_type=F32)


def z_line(parts, hz):
    first = lax.broadcasted_iota(jnp.int32, (128, 128), 1) < 64
    turned = [pltpu.roll(p, 64, 1) for p in parts]
    field = [
        jnp.concatenate([jnp.where(first, parts[s], turned[s + 1]) for s in (0, 2)], axis=1),
        jnp.concatenate([jnp.where(first, turned[s], parts[s + 1]) for s in (0, 2)], axis=1),
    ]
    high, low = split(jnp.concatenate(field, axis=0))
    return dot(high, hz[0]) + dot(high, hz[1]) + dot(low, hz[0])


def store(done, last, last_factor, hz, o_hbm, line, sems):
    ready = pl.ds(0, 15)
    bulk = pltpu.make_async_copy(done.at[:, ready], o_hbm.at[:, ready], sems.at[0])
    bulk.start()
    res = z_line([last[s] for s in range(4)], hz)
    for f in range(2):
        line[f] = res[128 * f : 128 * (f + 1)] * last_factor[...]
    tail = pltpu.make_async_copy(line, o_hbm.at[:, 15], sems.at[1])
    tail.start()
    bulk.wait()
    tail.wait()


def kernel(
    x_hbm, sx_hbm, sy_hbm, sz_hbm, h_hbm, hz_hbm, out, last, last_factor, hz_out,
    xin, h, hz, xo, zr, yr, yo, pr, fw, via, sx, sy, sz, sycol, factor,
    in_sem, tab_sem, sym_sem, sent, z_recv, xy_recv, p_recv, f_recv, v_recv, near, far, row, column,
):
    n = lax.axis_index("north")
    d = lax.axis_index("deep")
    half, q = n // PLANE, n % PLANE
    qx, qy = q % SIDE, q // SIDE
    group = 16 // PIECES

    def table_rows(rel, first, count):
        side = 1 - half if rel == 1 else half
        return pl.ds(pl.multiple_of(side * 256 + first, 128), count)

    def table_copy(k):
        rows = table_rows(*((0, 0, 256), (1, 0, 128), (1, 128, 128))[k])
        return pltpu.make_async_copy(h_hbm.at[:, rows], h.at[:, rows], tab_sem.at[k])

    hz_copy = pltpu.make_async_copy(hz_hbm, hz, sym_sem)
    table_copy(2).start()

    def in_copy(i, f):
        return pltpu.make_async_copy(x_hbm.at[f, pl.ds(2 * i, 2)], xin.at[pl.ds(2 * i, 2), f], in_sem.at[min(i, 1)])

    for f in range(2):
        in_copy(0, f).start()
    symbol_copies = [
        pltpu.make_async_copy(sx_hbm, sx, sym_sem),
        pltpu.make_async_copy(sy_hbm, sy, sym_sem),
        pltpu.make_async_copy(sz_hbm, sz, sym_sem),
    ]

    def plane_chip(step):
        return ((qy + step[1]) % SIDE) * SIDE + (qx + step[0]) % SIDE

    across = ((1 - half) * PLANE + q, d)
    mate, twin, beyond = (n, d ^ 2), (n, d ^ 1), ((1 - half) * PLANE + q, d ^ 2)
    middle = half != d // 2
    outer = half == d // 2

    def tell(semaphore, to):
        pl.semaphore_signal(semaphore, inc=1, device_id=to, device_id_type=MESH)

    barrier = pltpu.get_barrier_semaphore()
    for peer in (mate, twin):
        tell(barrier, peer)
    pl.when(middle)(lambda: tell(barrier, beyond))
    pl.when(qx > 0)(lambda: tell(barrier, (n - 1, d)))
    pl.when(qx < SIDE - 1)(lambda: tell(barrier, (n + 1, d)))
    pl.when(qy > 0)(lambda: tell(barrier, (n - SIDE, d)))
    pl.when(qy < SIDE - 1)(lambda: tell(barrier, (n + SIDE, d)))
    contacts = 2 + middle.astype(jnp.int32)
    for at in (qx, qy):
        contacts += (at > 0).astype(jnp.int32) + (at < SIDE - 1).astype(jnp.int32)

    def sweep(sems, at, stride):
        pl.when(at > 0)(lambda: pl.semaphore_wait(sems.at[0], 1))
        pl.when(at < SIDE - 1)(lambda: tell(sems.at[0], (n + stride, d)))
        pl.when(at < SIDE - 1)(lambda: pl.semaphore_wait(sems.at[1], 1))
        pl.when(at > 0)(lambda: tell(sems.at[1], (n - stride, d)))

    def z_copy(c, i, count):
        part = pl.ds(i, count)
        return pltpu.make_async_remote_copy(
            src_ref=xo.at[1, c, :, part],
            dst_ref=zr.at[c, :, part],
            send_sem=sent,
            recv_sem=z_recv.at[c, i // group],
            device_id=across,
            device_id_type=MESH,
        )


    def x_rows(i, high, low, rel, first, count):
        rows = table_rows(rel, first, count)
        a_high, a_low = h[0, rows, :], h[1, rows, :]
        res = dot(a_high, high, 1) + dot(a_low, high, 1) + dot(a_high, low, 1)
        for k in range(count // 128):
            part = res[128 * k : 128 * (k + 1)].reshape(PLANE, 8, 256)
            for y in range(2):
                xo[rel, first // 128 + k, :, 2 * i + y] = part[:, :, 128 * y : 128 * (y + 1)]

    def x_halves(i, *parts):
        high, low = split(xin[pl.ds(2 * i, 2)].reshape(256, 512))
        for part in parts:
            x_rows(i, high, low, *part)

    def x_step(i, carry):
        x_halves(i, (1, 0, 256), (0, 0, 256))
        z_copy(0, 2 * i, 2).start()
        return carry

    first_copy = pltpu.make_async_remote_copy(
        src_ref=xo.at[1, 1, :, pl.ds(0, 2)],
        dst_ref=via,
        send_sem=sent,
        recv_sem=v_recv,
        device_id=mate,
        device_id_type=MESH,
    )
    onward_copy = pltpu.make_async_remote_copy(
        src_ref=via,
        dst_ref=zr.at[1, :, pl.ds(0, 2)],
        send_sem=sent,
        recv_sem=z_recv.at[1, 0],
        device_id=beyond,
        device_id_type=MESH,
    )
    def in_wait(planes, k):
        pltpu.make_async_copy(xin.at[planes], xin.at[planes], in_sem.at[k]).wait()

    table_copy(2).wait()
    in_wait(pl.ds(0, 2), 0)
    table_copy(1).start()
    table_copy(0).start()
    for i in range(1, 8):
        for f in range(2):
            in_copy(i, f).start()
    for copy in [hz_copy, *symbol_copies]:
        copy.start()
    x_halves(0, (1, 128, 128))
    pl.semaphore_wait(barrier, contacts)
    first_copy.start()
    @pl.when(middle)
    def _():
        tell(near, mate)
        tell(near, beyond)

    table_copy(1).wait()
    x_halves(0, (1, 0, 128))
    pl.semaphore_wait(near, 1)
    z_copy(0, 0, 2).start()
    pl.when(middle)(lambda: tell(far, across))
    table_copy(0).wait()
    x_halves(0, (0, 0, 256))
    in_wait(pl.ds(2, 14), 1)
    lax.fori_loop(1, 4, x_step, 0)
    sweep(row, qx, 1)
    lax.fori_loop(4, 7, x_step, 0)
    sweep(column, qy, SIDE)
    x_step(7, 0)
    first_copy.wait_recv()
    pl.when(outer)(lambda: pl.semaphore_wait(far, 1))
    onward_copy.start()
    z_copy(1, 2, 2).start()
    for g in range(1, PIECES):
        z_copy(1, g * group, group).start()

    def xy_own(c):
        for step in STEPS:
            to = plane_chip(step)
            pltpu.make_async_remote_copy(
                src_ref=xo.at[0, c, to],
                dst_ref=yr.at[c, n],
                send_sem=sent,
                recv_sem=xy_recv.at[c],
                device_id=(half * PLANE + to, d),
                device_id_type=MESH,
            ).start()
        yr[c, n] = xo[0, c, q]

    from_across = (1 - half) * PLANE + q

    def xy_relay(c):
        def piece(k, carry):
            g = (k + c) % PIECES
            z_copy(c, g * group, group).wait_recv()
            part = pl.ds(g * group, group)
            for step in STEPS:
                to = plane_chip(step)
                pltpu.make_async_remote_copy(
                    src_ref=zr.at[c, to, part],
                    dst_ref=yr.at[c, from_across, part],
                    send_sem=sent,
                    recv_sem=xy_recv.at[c],
                    device_id=(half * PLANE + to, d),
                    device_id_type=MESH,
                ).start()
            return carry

        lax.fori_loop(0, PIECES, piece, 0)
        yr[c, from_across] = zr[c, q]

    def firsts(c):
        return range(0, 2, LINES[c])

    def p_copy(ref, source, c, j, to):
        part = pl.ds(j, LINES[c])
        return pltpu.make_async_remote_copy(
            src_ref=ref.at[part],
            dst_ref=pr.at[c, source, part],
            send_sem=sent,
            recv_sem=p_recv.at[c * 4 + j // LINES[c]],
            device_id=(n, to),
            device_id_type=MESH,
        )

    def to_twin(c, i):
        part = pl.ds(2 * i, 2)
        return pltpu.make_async_remote_copy(
            src_ref=yo.at[c, d ^ 3, part],
            dst_ref=fw.at[c, part],
            send_sem=sent,
            recv_sem=f_recv.at[c],
            device_id=(n, d ^ 1),
            device_id_type=MESH,
        )

    def onward(c):
        whole = fw.at[c]
        pltpu.make_async_remote_copy(
            src_ref=whole, dst_ref=whole, send_sem=sent, recv_sem=f_recv.at[c], device_id=twin, device_id_type=MESH
        ).wait_recv()

        def pair(i, carry):
            for j in firsts(c):
                p_copy(fw.at[c], d ^ 1, c, 2 * i + j, d ^ 2).start()
            return carry

        lax.fori_loop(0, 4, pair, 0)

    def along_y(c):
        pltpu.make_async_remote_copy(
            src_ref=yr.at[c, pl.ds(0, 30)],
            dst_ref=yr.at[c, pl.ds(0, 30)],
            send_sem=sent,
            recv_sem=xy_recv.at[c],
            device_id=across,
            device_id_type=MESH,
        ).wait_recv()
        lines = yr.at[c].reshape(4096, 128)

        def pair(i, carry):
            value = jnp.concatenate([lines[pl.ds(2 * i + k, 512, stride=8), :] for k in range(2)], axis=1)
            high, low = split(value)
            for part in range(2):
                rows = pl.ds(part * 256, 256)
                a_high, a_low = h[0, rows, :], h[1, rows, :]
                res = dot(a_high, high) + dot(a_low, high) + dot(a_high, low)
                res = jnp.swapaxes(res.reshape(2, PLANE, 8, 256), 0, 1).reshape(256, 256)
                for k in range(2):
                    for s in range(2):
                        yo[c, 2 * part + s, 2 * i + k] = res[128 * s : 128 * (s + 1), 128 * k : 128 * (k + 1)]
            pr[c, d, pl.ds(2 * i, 2)] = yo[c, d, pl.ds(2 * i, 2)]
            to_twin(c, i).start()
            for j in firsts(c):
                p_copy(yo.at[c, d ^ 1], d, c, 2 * i + j, d ^ 1).start()
                p_copy(yo.at[c, d ^ 2], d, c, 2 * i + j, d ^ 2).start()

            return carry

        lax.fori_loop(0, 4, pair, 0)
        onward(c)

    def line_factor(c, j):
        symbol = (sx[n * 16 + c * 8 + j] + sycol[...]) + sz[...]
        return (1.0 - 0.2 * symbol) / (1.0 + 0.2 * symbol)

    def line_wait(c, j):
        whole = pr.at[c, pl.ds(0, 3), pl.ds(0, LINES[c])]
        pltpu.make_async_remote_copy(
            src_ref=whole,
            dst_ref=whole,
            send_sem=sent,
            recv_sem=p_recv.at[c * 4 + j // LINES[c]],
            device_id=across,
            device_id_type=MESH,
        ).wait_recv()

    def along_z(c):
        def line(j, carry):
            factor[...] = line_factor(c, j)
            pl.when(j % LINES[c] == 0)(lambda: line_wait(c, j))
            res = z_line([pr[c, s, j] for s in range(4)], hz)
            for f in range(2):
                out[f, c * 8 + j] = res[128 * f : 128 * (f + 1)] * factor[...]
            return carry

        lax.fori_loop(0, 8 - c, line, 0)

    xy_own(0)
    xy_relay(0)
    xy_own(1)
    for copy in symbol_copies:
        copy.wait()
    hz_copy.wait()
    hz_out[...] = hz[...]
    along = sy[pl.ds(d, 1), :]
    sycol[...] = jnp.concatenate([jnp.transpose(jnp.broadcast_to(along, (128, 128)))] * 2, axis=1)
    along_y(0)
    xy_relay(1)
    along_y(1)
    along_z(0)
    along_z(1)
    last_factor[...] = line_factor(1, 7)
    line_wait(1, 7)
    for s in range(4):
        last[s] = pr[1, s, 7]

    def drain(ref, sem):
        pltpu.make_async_remote_copy(
            src_ref=ref, dst_ref=ref, send_sem=sem, recv_sem=p_recv.at[0], device_id=across, device_id_type=MESH
        ).wait_send()

    drain(via, sent)
    drain(zr, sent)
    for c in range(2):
        drain(yr.at[c, pl.ds(0, 30)], sent)
        drain(pr.at[c, pl.ds(0, 3)], sent)
        drain(fw.at[c], sent)


def local(forcing, symbol_x, symbol_y, symbol_z):
    lines = jnp.transpose(forcing, (0, 2, 3, 1))
    parts = pl.pallas_call(
        kernel,
        out_shape=[
            jax.ShapeDtypeStruct((2, 16, 128, 256), F32),
            jax.ShapeDtypeStruct((4, 128, 128), F32),
            jax.ShapeDtypeStruct((128, 256), F32),
            jax.ShapeDtypeStruct((2, 256, 256), BF16),
        ],
        in_specs=[pl.BlockSpec(memory_space=pltpu.HBM)] * 6,
        out_specs=[pl.BlockSpec(memory_space=pltpu.VMEM)] * 4,
        scratch_shapes=[
            pltpu.VMEM((16, 2, 64, 512), F32),
            pltpu.VMEM((2, 512, 512), BF16),
            pltpu.VMEM((2, 256, 256), BF16),
            pltpu.VMEM((2, 2, 16, 16, 8, 128), F32),
            pltpu.VMEM((2, 16, 16, 8, 128), F32),
            pltpu.VMEM((2, 32, 16, 8, 128), F32),
            pltpu.VMEM((2, 4, 8, 128, 128), F32),
            pltpu.VMEM((2, 4, 8, 128, 128), F32),
            pltpu.VMEM((2, 8, 128, 128), F32),
            pltpu.VMEM((16, 2, 8, 128), F32),
            pltpu.SMEM((512,), F32),
            pltpu.VMEM((4, 128), F32),
            pltpu.VMEM((1, 256), F32),
            pltpu.VMEM((128, 256), F32),
            pltpu.VMEM((128, 256), F32),
            pltpu.SemaphoreType.DMA((2,)),
            pltpu.SemaphoreType.DMA((3,)),
            pltpu.SemaphoreType.DMA,
            pltpu.SemaphoreType.DMA,
            pltpu.SemaphoreType.DMA((2, PIECES)),
            pltpu.SemaphoreType.DMA((2,)),
            pltpu.SemaphoreType.DMA((12,)),
            pltpu.SemaphoreType.DMA((2,)),
            pltpu.SemaphoreType.DMA,
            pltpu.SemaphoreType.REGULAR,
            pltpu.SemaphoreType.REGULAR,
            pltpu.SemaphoreType.REGULAR((2,)),
            pltpu.SemaphoreType.REGULAR((2,)),
        ],
        compiler_params=pltpu.CompilerParams(
            collective_id=0, has_side_effects=True, vmem_limit_bytes=48 * 2**20
        ),
        name="transform",
    )(
        *(
            pltpu.with_memory_space_constraint(value, pltpu.HBM)
            for value in (
                lines,
                symbol_x,
                symbol_y.reshape(4, 128),
                symbol_z.reshape(1, 256),
                jnp.asarray(by_chunk(table(512))),
                jnp.asarray(table(256)),
            )
        )
    )

    return pl.pallas_call(
        store,
        out_shape=jax.ShapeDtypeStruct((2, 16, 128, 256), F32),
        in_specs=[pl.BlockSpec(memory_space=pl.ANY)] + [pl.BlockSpec(memory_space=pltpu.VMEM)] * 3,
        out_specs=pl.BlockSpec(memory_space=pltpu.HBM),
        scratch_shapes=[pltpu.VMEM((2, 128, 256), F32), pltpu.SemaphoreType.DMA((2,))],
        compiler_params=pltpu.CompilerParams(vmem_limit_bytes=8 * 2**20),
        name="store",
    )(*parts)


def solution(mesh):
    return jax.shard_map(
        local,
        mesh=mesh,
        in_specs=(P(None, None, "north", "deep"), P(), P(), P()),
        out_specs=P(None, "north", "deep", None),
        check_vma=False,
    )
```

```python
import functools

import jax
import jax.numpy as jnp
import ml_dtypes
import numpy as np
from jax import lax
from jax.experimental import pallas as pl
from jax.experimental.pallas import tpu as pltpu
from jax.sharding import PartitionSpec as P

MESH = pl.DeviceIdType.MESH
F32, BF16 = jnp.float32, jnp.bfloat16
SIDE = 4
PLANE = SIDE * SIDE
STEPS = ((1, 0), (0, 1), (3, 0), (0, 3), (1, 1), (3, 3), (1, 3), (3, 1), (2, 0), (0, 2), (2, 1), (1, 2), (2, 3), (3, 2), (2, 2))
LINE = tuple(step for step in STEPS if 0 in step)
PIECES = 2

LINES = (2, 1)


def table(count):
    rank = np.arange(count, dtype=np.int64)
    turns = ((2 * rank[:, None] + 1) * (2 * rank[None, :] + 1)) % (8 * count)
    exact = np.cos(np.pi / (4 * count) * turns) * np.sqrt(2.0 / count)
    high = exact.astype(np.float32).astype(ml_dtypes.bfloat16)
    low = (exact - high.astype(np.float64)).astype(np.float32).astype(ml_dtypes.bfloat16)
    return np.stack([high, low])


def by_chunk(rows):
    parts = rows.reshape(2, 2, PLANE, 2, 8, rows.shape[-1])
    return np.ascontiguousarray(parts.transpose(0, 1, 3, 2, 4, 5)).reshape(rows.shape)


def split(value):
    high = value.astype(BF16)
    return high, (value - high.astype(F32)).astype(BF16)


def dot(a, b, b_dim=0):
    return lax.dot_general(a, b, (((1,), (b_dim,)), ((), ())), preferred_element_type=F32)


def z_line(parts, hz):
    first = lax.broadcasted_iota(jnp.int32, (128, 128), 1) < 64
    turned = [pltpu.roll(p, 64, 1) for p in parts]
    field = [
        jnp.concatenate([jnp.where(first, parts[s], turned[s + 1]) for s in (0, 2)], axis=1),
        jnp.concatenate([jnp.where(first, turned[s], parts[s + 1]) for s in (0, 2)], axis=1),
    ]
    high, low = split(jnp.concatenate(field, axis=0))
    return dot(high, hz[0]) + dot(high, hz[1]) + dot(low, hz[0])


def store(done, last, last_factor, hz, o_hbm, line, sems):
    ready = pl.ds(0, 15)
    bulk = pltpu.make_async_copy(done.at[:, ready], o_hbm.at[:, ready], sems.at[0])
    bulk.start()
    res = z_line([last[s] for s in range(4)], hz)
    for f in range(2):
        line[f] = res[128 * f : 128 * (f + 1)] * last_factor[...]
    tail = pltpu.make_async_copy(line, o_hbm.at[:, 15], sems.at[1])
    tail.start()
    bulk.wait()
    tail.wait()


def kernel(
    x_hbm, sx_hbm, sy_hbm, sz_hbm, h_hbm, hz_hbm, out, last, last_factor, hz_out,
    xin, h, hz, xo, zr, yr, yo, pr, fw, via, sx, sy, sz, sycol, factor,
    in_sem, tab_sem, sym_sem, sent, z_recv, xy_recv, p_recv, f_recv, v_recv, near, far, row, column,
):
    n = lax.axis_index("north")
    d = lax.axis_index("deep")
    half, q = n // PLANE, n % PLANE
    qx, qy = q % SIDE, q // SIDE
    group = 16 // PIECES

    def table_rows(rel, first, count):
        side = 1 - half if rel == 1 else half
        return pl.ds(pl.multiple_of(side * 256 + first, 128), count)

    def table_copy(k):
        rows = table_rows(*((0, 0, 256), (1, 0, 128), (1, 128, 128))[k])
        return pltpu.make_async_copy(h_hbm.at[:, rows], h.at[:, rows], tab_sem.at[k])

    hz_copy = pltpu.make_async_copy(hz_hbm, hz, sym_sem)
    table_copy(2).start()

    def in_copy(i, f):
        return pltpu.make_async_copy(x_hbm.at[f, pl.ds(2 * i, 2)], xin.at[pl.ds(2 * i, 2), f], in_sem.at[min(i, 1)])

    for f in range(2):
        in_copy(0, f).start()
    symbol_copies = [
        pltpu.make_async_copy(sx_hbm, sx, sym_sem),
        pltpu.make_async_copy(sy_hbm, sy, sym_sem),
        pltpu.make_async_copy(sz_hbm, sz, sym_sem),
    ]

    def plane_chip(step):
        return ((qy + step[1]) % SIDE) * SIDE + (qx + step[0]) % SIDE

    across = ((1 - half) * PLANE + q, d)
    mate, twin, beyond = (n, d ^ 2), (n, d ^ 1), ((1 - half) * PLANE + q, d ^ 2)
    middle = half != d // 2
    outer = half == d // 2

    def tell(semaphore, to):
        pl.semaphore_signal(semaphore, inc=1, device_id=to, device_id_type=MESH)

    barrier = pltpu.get_barrier_semaphore()
    for peer in (mate, twin):
        tell(barrier, peer)
    pl.when(middle)(lambda: tell(barrier, beyond))
    pl.when(qx > 0)(lambda: tell(barrier, (n - 1, d)))
    pl.when(qx < SIDE - 1)(lambda: tell(barrier, (n + 1, d)))
    pl.when(qy > 0)(lambda: tell(barrier, (n - SIDE, d)))
    pl.when(qy < SIDE - 1)(lambda: tell(barrier, (n + SIDE, d)))
    contacts = 2 + middle.astype(jnp.int32)
    for at in (qx, qy):
        contacts += (at > 0).astype(jnp.int32) + (at < SIDE - 1).astype(jnp.int32)

    def sweep(sems, at, stride):
        pl.when(at > 0)(lambda: pl.semaphore_wait(sems.at[0], 1))
        pl.when(at < SIDE - 1)(lambda: tell(sems.at[0], (n + stride, d)))
        pl.when(at < SIDE - 1)(lambda: pl.semaphore_wait(sems.at[1], 1))
        pl.when(at > 0)(lambda: tell(sems.at[1], (n - stride, d)))

    def z_copy(c, i, count):
        part = pl.ds(i, count)
        return pltpu.make_async_remote_copy(
            src_ref=xo.at[1, c, :, part],
            dst_ref=zr.at[c, :, part],
            send_sem=sent,
            recv_sem=z_recv.at[c, i // group],
            device_id=across,
            device_id_type=MESH,
        )


    def x_rows(i, high, low, rel, first, count):
        rows = table_rows(rel, first, count)
        a_high, a_low = h[0, rows, :], h[1, rows, :]
        res = dot(a_high, high, 1) + dot(a_low, high, 1) + dot(a_high, low, 1)
        for k in range(count // 128):
            part = res[128 * k : 128 * (k + 1)].reshape(PLANE, 8, 256)
            for y in range(2):
                xo[rel, first // 128 + k, :, 2 * i + y] = part[:, :, 128 * y : 128 * (y + 1)]

    def x_halves(i, *parts):
        high, low = split(xin[pl.ds(2 * i, 2)].reshape(256, 512))
        for part in parts:
            x_rows(i, high, low, *part)

    def x_step(i, carry):
        x_halves(i, (1, 0, 256), (0, 0, 256))
        z_copy(0, 2 * i, 2).start()
        return carry

    first_copy = pltpu.make_async_remote_copy(
        src_ref=xo.at[1, 1, :, pl.ds(0, 2)],
        dst_ref=via,
        send_sem=sent,
        recv_sem=v_recv,
        device_id=mate,
        device_id_type=MESH,
    )
    onward_copy = pltpu.make_async_remote_copy(
        src_ref=via,
        dst_ref=zr.at[1, :, pl.ds(0, 2)],
        send_sem=sent,
        recv_sem=z_recv.at[1, 0],
        device_id=beyond,
        device_id_type=MESH,
    )
    def in_wait(planes, k):
        pltpu.make_async_copy(xin.at[planes], xin.at[planes], in_sem.at[k]).wait()

    table_copy(2).wait()
    in_wait(pl.ds(0, 2), 0)
    table_copy(1).start()
    table_copy(0).start()
    for i in range(1, 8):
        for f in range(2):
            in_copy(i, f).start()
    for copy in [hz_copy, *symbol_copies]:
        copy.start()
    x_halves(0, (1, 128, 128))
    pl.semaphore_wait(barrier, contacts)
    first_copy.start()
    @pl.when(middle)
    def _():
        tell(near, mate)
        tell(near, beyond)

    table_copy(1).wait()
    x_halves(0, (1, 0, 128))
    pl.semaphore_wait(near, 1)
    z_copy(0, 0, 2).start()
    pl.when(middle)(lambda: tell(far, across))
    table_copy(0).wait()
    x_halves(0, (0, 0, 256))
    in_wait(pl.ds(2, 14), 1)
    lax.fori_loop(1, 4, x_step, 0)
    sweep(row, qx, 1)
    lax.fori_loop(4, 7, x_step, 0)
    sweep(column, qy, SIDE)
    x_step(7, 0)
    first_copy.wait_recv()
    pl.when(outer)(lambda: pl.semaphore_wait(far, 1))
    onward_copy.start()
    z_copy(1, 2, group - 2).start()
    for g in range(1, PIECES):
        z_copy(1, g * group, group).start()

    def xy_own(c):
        for step in STEPS:
            to = plane_chip(step)
            pltpu.make_async_remote_copy(
                src_ref=xo.at[0, c, to],
                dst_ref=yr.at[c, n],
                send_sem=sent,
                recv_sem=xy_recv.at[c],
                device_id=(half * PLANE + to, d),
                device_id_type=MESH,
            ).start()
        yr[c, n] = xo[0, c, q]

    from_across = (1 - half) * PLANE + q

    def xy_relay(c):
        def piece(k, carry):
            g = (k + c) % PIECES
            z_copy(c, g * group, group).wait_recv()
            part = pl.ds(g * group, group)
            for step in STEPS:
                to = plane_chip(step)
                pltpu.make_async_remote_copy(
                    src_ref=zr.at[c, to, part],
                    dst_ref=yr.at[c, from_across, part],
                    send_sem=sent,
                    recv_sem=xy_recv.at[c],
                    device_id=(half * PLANE + to, d),
                    device_id_type=MESH,
                ).start()
            return carry

        lax.fori_loop(0, PIECES, piece, 0)
        yr[c, from_across] = zr[c, q]

    def firsts(c):
        return range(0, 2, LINES[c])

    def p_copy(ref, source, c, j, to):
        part = pl.ds(j, LINES[c])
        return pltpu.make_async_remote_copy(
            src_ref=ref.at[part],
            dst_ref=pr.at[c, source, part],
            send_sem=sent,
            recv_sem=p_recv.at[c * 4 + j // LINES[c]],
            device_id=(n, to),
            device_id_type=MESH,
        )

    def to_twin(c, i):
        part = pl.ds(2 * i, 2)
        return pltpu.make_async_remote_copy(
            src_ref=yo.at[c, d ^ 3, part],
            dst_ref=fw.at[c, part],
            send_sem=sent,
            recv_sem=f_recv.at[c],
            device_id=(n, d ^ 1),
            device_id_type=MESH,
        )

    def onward(c):
        whole = fw.at[c]
        pltpu.make_async_remote_copy(
            src_ref=whole, dst_ref=whole, send_sem=sent, recv_sem=f_recv.at[c], device_id=twin, device_id_type=MESH
        ).wait_recv()

        def pair(i, carry):
            for j in firsts(c):
                p_copy(fw.at[c], d ^ 1, c, 2 * i + j, d ^ 2).start()
            return carry

        lax.fori_loop(0, 4, pair, 0)

    def along_y(c):
        pltpu.make_async_remote_copy(
            src_ref=yr.at[c, pl.ds(0, 30)],
            dst_ref=yr.at[c, pl.ds(0, 30)],
            send_sem=sent,
            recv_sem=xy_recv.at[c],
            device_id=across,
            device_id_type=MESH,
        ).wait_recv()
        lines = yr.at[c].reshape(4096, 128)

        def pair(i, carry):
            value = jnp.concatenate([lines[pl.ds(2 * i + k, 512, stride=8), :] for k in range(2)], axis=1)
            high, low = split(value)
            for part in range(2):
                rows = pl.ds(part * 256, 256)
                a_high, a_low = h[0, rows, :], h[1, rows, :]
                res = dot(a_high, high) + dot(a_low, high) + dot(a_high, low)
                res = jnp.swapaxes(res.reshape(2, PLANE, 8, 256), 0, 1).reshape(256, 256)
                for k in range(2):
                    for s in range(2):
                        yo[c, 2 * part + s, 2 * i + k] = res[128 * s : 128 * (s + 1), 128 * k : 128 * (k + 1)]
            pr[c, d, pl.ds(2 * i, 2)] = yo[c, d, pl.ds(2 * i, 2)]
            to_twin(c, i).start()
            for j in firsts(c):
                p_copy(yo.at[c, d ^ 1], d, c, 2 * i + j, d ^ 1).start()
                p_copy(yo.at[c, d ^ 2], d, c, 2 * i + j, d ^ 2).start()

            return carry

        lax.fori_loop(0, 4, pair, 0)
        onward(c)

    def line_factor(c, j):
        symbol = (sx[n * 16 + c * 8 + j] + sycol[...]) + sz[...]
        return (1.0 - 0.2 * symbol) / (1.0 + 0.2 * symbol)

    def line_wait(c, j):
        whole = pr.at[c, pl.ds(0, 3), pl.ds(0, LINES[c])]
        pltpu.make_async_remote_copy(
            src_ref=whole,
            dst_ref=whole,
            send_sem=sent,
            recv_sem=p_recv.at[c * 4 + j // LINES[c]],
            device_id=across,
            device_id_type=MESH,
        ).wait_recv()

    def along_z(c):
        def line(j, carry):
            factor[...] = line_factor(c, j)
            pl.when(j % LINES[c] == 0)(lambda: line_wait(c, j))
            res = z_line([pr[c, s, j] for s in range(4)], hz)
            for f in range(2):
                out[f, c * 8 + j] = res[128 * f : 128 * (f + 1)] * factor[...]
            return carry

        lax.fori_loop(0, 8 - c, line, 0)

    xy_own(0)
    xy_relay(0)
    xy_own(1)
    for copy in symbol_copies:
        copy.wait()
    hz_copy.wait()
    hz_out[...] = hz[...]
    along = sy[pl.ds(d, 1), :]
    sycol[...] = jnp.concatenate([jnp.transpose(jnp.broadcast_to(along, (128, 128)))] * 2, axis=1)
    along_y(0)
    xy_relay(1)
    along_y(1)
    along_z(0)
    along_z(1)
    last_factor[...] = line_factor(1, 7)
    line_wait(1, 7)
    for s in range(4):
        last[s] = pr[1, s, 7]

    def drain(ref, sem):
        pltpu.make_async_remote_copy(
            src_ref=ref, dst_ref=ref, send_sem=sem, recv_sem=p_recv.at[0], device_id=across, device_id_type=MESH
        ).wait_send()

    drain(via, sent)
    drain(zr, sent)
    for c in range(2):
        drain(yr.at[c, pl.ds(0, 30)], sent)
        drain(pr.at[c, pl.ds(0, 3)], sent)
        drain(fw.at[c], sent)


def local(forcing, symbol_x, symbol_y, symbol_z):
    lines = jnp.transpose(forcing, (0, 2, 3, 1))
    parts = pl.pallas_call(
        kernel,
        out_shape=[
            jax.ShapeDtypeStruct((2, 16, 128, 256), F32),
            jax.ShapeDtypeStruct((4, 128, 128), F32),
            jax.ShapeDtypeStruct((128, 256), F32),
            jax.ShapeDtypeStruct((2, 256, 256), BF16),
        ],
        in_specs=[pl.BlockSpec(memory_space=pltpu.HBM)] * 6,
        out_specs=[pl.BlockSpec(memory_space=pltpu.VMEM)] * 4,
        scratch_shapes=[
            pltpu.VMEM((16, 2, 64, 512), F32),
            pltpu.VMEM((2, 512, 512), BF16),
            pltpu.VMEM((2, 256, 256), BF16),
            pltpu.VMEM((2, 2, 16, 16, 8, 128), F32),
            pltpu.VMEM((2, 16, 16, 8, 128), F32),
            pltpu.VMEM((2, 32, 16, 8, 128), F32),
            pltpu.VMEM((2, 4, 8, 128, 128), F32),
            pltpu.VMEM((2, 4, 8, 128, 128), F32),
            pltpu.VMEM((2, 8, 128, 128), F32),
            pltpu.VMEM((16, 2, 8, 128), F32),
            pltpu.SMEM((512,), F32),
            pltpu.VMEM((4, 128), F32),
            pltpu.VMEM((1, 256), F32),
            pltpu.VMEM((128, 256), F32),
            pltpu.VMEM((128, 256), F32),
            pltpu.SemaphoreType.DMA((2,)),
            pltpu.SemaphoreType.DMA((3,)),
            pltpu.SemaphoreType.DMA,
            pltpu.SemaphoreType.DMA,
            pltpu.SemaphoreType.DMA((2, PIECES)),
            pltpu.SemaphoreType.DMA((2,)),
            pltpu.SemaphoreType.DMA((12,)),
            pltpu.SemaphoreType.DMA((2,)),
            pltpu.SemaphoreType.DMA,
            pltpu.SemaphoreType.REGULAR,
            pltpu.SemaphoreType.REGULAR,
            pltpu.SemaphoreType.REGULAR((2,)),
            pltpu.SemaphoreType.REGULAR((2,)),
        ],
        compiler_params=pltpu.CompilerParams(
            collective_id=0, has_side_effects=True, vmem_limit_bytes=48 * 2**20
        ),
        name="transform",
    )(
        *(
            pltpu.with_memory_space_constraint(value, pltpu.HBM)
            for value in (
                lines,
                symbol_x,
                symbol_y.reshape(4, 128),
                symbol_z.reshape(1, 256),
                jnp.asarray(by_chunk(table(512))),
                jnp.asarray(table(256)),
            )
        )
    )

    return pl.pallas_call(
        store,
        out_shape=jax.ShapeDtypeStruct((2, 16, 128, 256), F32),
        in_specs=[pl.BlockSpec(memory_space=pl.ANY)] + [pl.BlockSpec(memory_space=pltpu.VMEM)] * 3,
        out_specs=pl.BlockSpec(memory_space=pltpu.HBM),
        scratch_shapes=[pltpu.VMEM((2, 128, 256), F32), pltpu.SemaphoreType.DMA((2,))],
        compiler_params=pltpu.CompilerParams(vmem_limit_bytes=8 * 2**20),
        name="store",
    )(*parts)


def solution(mesh):
    return jax.shard_map(
        local,
        mesh=mesh,
        in_specs=(P(None, None, "north", "deep"), P(), P(), P()),
        out_specs=P(None, "north", "deep", None),
        check_vma=False,
    )
```
